32 devices in a mesh: data: 4 (over y, z), model: 8 (over x, core).
Axes of the slice: x: 4, y: 2, z: 2, core: 2. Of those that a mesh axis runs over, the one named last changes fastest.
The devices are a block of a 4x4x8 slice.
Arguments:
- x: bfloat16 [768, 16, 1024], P('data'), parts along dimension 0
- w_in: bfloat16 [1024, 4, 8192], P(None, None, 'model')
- w_rec: bfloat16 [8192, 4, 8192], P(None, None, 'model')
- gate_bias: float32 [4, 8192], P(None, 'model')
- h_init: float32 [768, 8192], P('data', 'model'), parts along dimension 0
- c_init: float32 [768, 8192], P('data', 'model'), parts along dimension 0
Outputs:
- output 1: bfloat16 [768, 16, 8192], P('data', None, 'model'), parts along dimension 0
- output 2: float32 [768, 8192], P('data', 'model'), parts along dimension 0
- output 3: float32 [768, 8192], P('data', 'model'), parts along dimension 0
There are 4 independent parts. The reference program is written for one: setup_inputs(seed, part) draws one part's arguments, and reference() takes and returns one part's arrays. A program takes and returns all parts, laid end to end along the dimension named above; an argument that names none is the same for every part.
All inputs are finite; a program needn't handle non-finite values.
Results may differ from the reference program's by a relative error of at most 0.00305013.
Values are sent between devices in bfloat16 or wider.
A program may use at most 768 MiB of HBM per device.

```python
import jax
import jax.numpy as jnp
from jax import lax

BATCH_ROWS = 192
TIME_STEPS = 16
INPUT_DIM = 1024
HIDDEN_DIM = 8192


def setup_inputs(seed: int = 0, part: int = 0) -> dict:
    part_keys = jax.random.split(jax.random.fold_in(jax.random.key(seed), part), 3)
    shared_keys = jax.random.split(jax.random.key(seed + 1), 3)
    x = jax.random.normal(part_keys[0], (BATCH_ROWS, TIME_STEPS, INPUT_DIM), jnp.float32)
    h_init = jnp.tanh(jax.random.normal(part_keys[1], (BATCH_ROWS, HIDDEN_DIM), jnp.float32))
    c_init = jax.random.normal(part_keys[2], (BATCH_ROWS, HIDDEN_DIM), jnp.float32)
    w_in = jax.random.normal(shared_keys[0], (INPUT_DIM, 4, HIDDEN_DIM), jnp.float32) * (INPUT_DIM ** -0.5)
    w_rec = jax.random.normal(shared_keys[1], (HIDDEN_DIM, 4, HIDDEN_DIM), jnp.float32) * (1.5 * HIDDEN_DIM ** -0.5)
    offsets = jnp.array([0.0, 3.0, 0.0, 0.0], jnp.float32)[:, None]
    gate_bias = 0.5 * jax.random.normal(shared_keys[2], (4, HIDDEN_DIM), jnp.float32) + offsets
    return {
        "x": x.astype(jnp.bfloat16),
        "w_in": w_in.astype(jnp.bfloat16),
        "w_rec": w_rec.astype(jnp.bfloat16),
        "gate_bias": gate_bias,
        "h_init": h_init,
        "c_init": c_init,
    }


def reference(x, w_in, w_rec, gate_bias, h_init, c_init):
    in_dim = w_in.shape[0]
    hidden = w_rec.shape[0]
    batch_rows = x.shape[0]
    w_in_flat = w_in.reshape(in_dim, 4 * hidden)
    w_rec_flat = w_rec.reshape(hidden, 4 * hidden)

    def step_fn(carry_in, x_step):
        h_prev, c_prev = carry_in
        gate_pre = jnp.dot(x_step, w_in_flat, preferred_element_type=jnp.float32) + jnp.dot(
            h_prev.astype(jnp.bfloat16), w_rec_flat, preferred_element_type=jnp.float32)
        gate_pre = gate_pre.reshape(batch_rows, 4, hidden) + gate_bias
        c_next = jax.nn.sigmoid(gate_pre[:, 1]) * c_prev + jax.nn.sigmoid(gate_pre[:, 0]) * jnp.tanh(gate_pre[:, 3])
        h_next = jax.nn.sigmoid(gate_pre[:, 2]) * jnp.tanh(c_next)
        return (h_next, c_next), h_next.astype(jnp.bfloat16)

    (h_last, c_last), y_steps = lax.scan(step_fn, (h_init, c_init), jnp.swapaxes(x, 0, 1))
    return jnp.swapaxes(y_steps, 0, 1), h_last, c_last
```

```python
import functools

import jax
import jax.numpy as jnp
from jax import lax
from jax.experimental import pallas as pl
from jax.experimental.pallas import tpu as pltpu
from jax.sharding import PartitionSpec as P

CORES = 2
CHUNKS = 4
NSLOT = 3

RIGHT, LEFT, PARTNER, P_RIGHT, P_LEFT, OPPOSITE, P_OPPOSITE = range(7)


def lstm_kernel(n, steps, x_ref, wx_ref, wh_ref, bias_ref, h0_ref, c0_ref,
                y_ref, hl_ref, cl_ref,
                hbuf, wres, wstr, acc, cst, send_sem, recv_sem, res_sem, str_sem, loc_sem, y_sem, x_sem):
    rows, half = hbuf.shape[1], hbuf.shape[2]
    units = 2 * half
    piece = units // CHUNKS
    chips = n // CORES
    nblk = n + 1
    me = lax.axis_index("model")
    chip, core = me // CORES, me % CORES
    other = 1 - core
    right_chip, left_chip = (chip + 1) % chips, (chip + chips - 1) % chips
    far_chip = (chip + 2) % chips
    own = chip * CORES + core
    partner = chip * CORES + other
    right = right_chip * CORES + core
    left = left_chip * CORES + core
    p_right = right_chip * CORES + other
    p_left = left_chip * CORES + other
    far = far_chip * CORES + core
    p_far = far_chip * CORES + other

    passes = [
        ((None, 0), (None, 1)),
        ((own, 0), (own, 1)),
        ((partner, 0), (partner, 1)),
        ((right, 0), (left, 0)),
        ((right, 1), (left, 1)),
        ((p_right, 0), (p_left, 0)),
        ((p_right, 1), (p_left, 1)),
        ((far, 0), (far, 1)),
        ((p_far, 0), (p_far, 1)),
    ]
    npass = len(passes)

    def weight_src(part):
        blk, hf = part
        if blk is None:
            return wx_ref.at[pl.ds(hf * half, half)]
        return wh_ref.at[pl.ds(pl.multiple_of(blk * units + hf * half, half), half)]

    def hidx(slot, blk, hf):
        return (slot * nblk + (n if blk is None else blk)) * 2 + hf

    def resident(j):
        return pltpu.make_async_copy(weight_src(passes[j][0]), wres.at[j], res_sem.at[j])

    def streamed(j):
        return pltpu.make_async_copy(weight_src(passes[j][1]), wstr.at[j % NSLOT], str_sem.at[j % NSLOT])

    def x_copies(t, slot):
        return [
            pltpu.make_async_copy(x_ref.at[t, :, pl.ds(hf * half, half)], hbuf.at[hidx(slot, None, hf)], x_sem.at[hf])
            for hf in range(2)
        ]

    def y_copies(t, slot):
        return [
            pltpu.make_async_copy(hbuf.at[hidx(slot, own, hf)], y_ref.at[t, :, pl.ds(hf * half, half)], y_sem.at[hf])
            for hf in range(2)
        ]

    def remote(kind, c, slot):
        src_blk = {RIGHT: own, LEFT: own, PARTNER: own, P_RIGHT: right, P_LEFT: left,
                   OPPOSITE: right if c % 2 == 0 else left, P_OPPOSITE: far}[kind]
        dst = {RIGHT: left, LEFT: right, PARTNER: partner, P_RIGHT: partner, P_LEFT: partner,
               OPPOSITE: left if c % 2 == 0 else right, P_OPPOSITE: partner}[kind]
        view = hbuf.at[hidx(slot, src_blk, c // 2), :, pl.ds((c % 2) * piece, piece)]
        return pltpu.make_async_remote_copy(
            src_ref=view, dst_ref=view, send_sem=send_sem.at[kind, c], recv_sem=recv_sem.at[slot, kind, c],
            device_id={"model": dst}, device_id_type=pl.DeviceIdType.MESH)

    def arrive(kind, c, slot):
        blk = {RIGHT: right, LEFT: left, PARTNER: partner, P_RIGHT: p_right, P_LEFT: p_left,
               OPPOSITE: far, P_OPPOSITE: p_far}[kind]
        view = hbuf.at[hidx(slot, blk, c // 2), :, pl.ds((c % 2) * piece, piece)]
        pltpu.make_async_remote_copy(
            src_ref=view, dst_ref=view, send_sem=send_sem.at[kind, c], recv_sem=recv_sem.at[slot, kind, c],
            device_id={"model": partner}, device_id_type=pl.DeviceIdType.MESH).wait_recv()

    def send_own(c, slot):
        for kind in (RIGHT, LEFT, PARTNER):
            remote(kind, c, slot).start()

    def pass_on(c, slot):
        arrive(RIGHT, c, slot)
        if c % 2 == 0:
            remote(OPPOSITE, c, slot).start()
        remote(P_RIGHT, c, slot).start()
        arrive(LEFT, c, slot)
        if c % 2 == 1:
            remote(OPPOSITE, c, slot).start()
        remote(P_LEFT, c, slot).start()

    def sends_done(slot):
        for kind in range(7):
            for c in range(CHUNKS):
                remote(kind, c, slot).wait_send()

    h0_copy = pltpu.make_async_copy(h0_ref, acc.at[:, pl.ds(0, units)], loc_sem.at[0])
    c0_copy = pltpu.make_async_copy(c0_ref, cst, loc_sem.at[1])
    h0_copy.start()
    c0_copy.start()
    for cp in x_copies(0, 0):
        cp.start()
    for j in range(npass):
        resident(j).start()
        if j < NSLOT:
            streamed(j).start()

    barrier = pltpu.get_barrier_semaphore()
    for peer in (left, right, partner):
        pl.semaphore_signal(barrier, inc=1, device_id={"model": peer}, device_id_type=pl.DeviceIdType.MESH)
    pl.semaphore_wait(barrier, 3)

    h0_copy.wait()
    for hf in range(2):
        hbuf[hidx(0, own, hf)] = acc[:, hf * half:(hf + 1) * half].astype(jnp.bfloat16)
    for c in range(CHUNKS):
        send_own(c, 0)
    c0_copy.wait()

    def accumulate(j, slot):
        (ba, ha), (bb, hb) = passes[j]
        ia, ib = hidx(slot, ba, ha), hidx(slot, bb, hb)
        ntile = half
        for k in range(4 * units // ntile):
            cols = slice(k * ntile, (k + 1) * ntile)
            add = jnp.dot(hbuf[ia], wres[j, :, cols], preferred_element_type=jnp.float32)
            add += jnp.dot(hbuf[ib], wstr[j % NSLOT, :, cols], preferred_element_type=jnp.float32)
            if j == 0:
                acc[:, cols] = add + bias_ref[:, cols]
            else:
                acc[:, cols] += add

    def finish(c, slot, nxt):
        parts = []
        for j in (npass - 2, npass - 1):
            (ba, ha), (bb, hb) = passes[j]
            parts.append((hidx(slot, ba, ha), wres, j))
            parts.append((hidx(slot, bb, hb), wstr, j % NSLOT))
        for g in range(4):
            cols = slice(g * units + c * piece, g * units + (c + 1) * piece)
            add = None
            for ih, wref, jw in parts:
                term = jnp.dot(hbuf[ih], wref[jw, :, cols], preferred_element_type=jnp.float32)
                add = term if add is None else add + term
            acc[:, cols] += add
        own_idx = hidx(nxt, own, c // 2)
        rblk = 16
        for r in range(rows // rblk):
            rs = slice(r * rblk, (r + 1) * rblk)
            us = slice(c * piece, (c + 1) * piece)
            gi, gf, go, gu = (acc[rs, g * units + c * piece:g * units + (c + 1) * piece] for g in range(4))
            si = 0.5 * jnp.tanh(0.5 * gi) + 0.5
            sf = 0.5 * jnp.tanh(0.5 * gf) + 0.5
            so = 0.5 * jnp.tanh(0.5 * go) + 0.5
            cn = sf * cst[rs, us] + si * jnp.tanh(gu)
            hn = so * jnp.tanh(cn)
            cst[rs, us] = cn
            acc[rs, us] = hn
            hbuf[own_idx, rs, (c % 2) * piece:(c % 2 + 1) * piece] = hn.astype(jnp.bfloat16)

    def step(t, carry):
        slot = t % 2
        nxt = 1 - slot
        first, last = t == 0, t == steps - 1

        def weights(j):
            @pl.when(first)
            def _():
                resident(j).wait()
            streamed(j).wait()

        def refill(j):
            k = j + NSLOT
            if k < npass:
                streamed(k).start()
            else:
                @pl.when(jnp.logical_not(last))
                def _():
                    streamed(k - npass).start()

        for cp in x_copies(t, slot):
            cp.wait()
        weights(0)
        accumulate(0, slot)
        refill(0)
        weights(1)
        accumulate(1, slot)
        refill(1)
        pass_on(0, slot)
        pass_on(1, slot)
        for c in range(CHUNKS):
            arrive(PARTNER, c, slot)
        weights(2)
        accumulate(2, slot)
        refill(2)
        pass_on(2, slot)
        weights(3)
        accumulate(3, slot)
        refill(3)
        pass_on(3, slot)
        weights(4)
        accumulate(4, slot)
        refill(4)
        for c in range(2):
            arrive(P_RIGHT, c, slot)
            arrive(P_LEFT, c, slot)
        weights(5)
        accumulate(5, slot)
        refill(5)
        for c in range(CHUNKS):
            arrive(OPPOSITE, c, slot)
            remote(P_OPPOSITE, c, slot).start()
        for c in range(2, CHUNKS):
            arrive(P_RIGHT, c, slot)
            arrive(P_LEFT, c, slot)
        weights(6)
        accumulate(6, slot)
        refill(6)
        weights(7)
        weights(8)
        for c in range(CHUNKS):
            arrive(P_OPPOSITE, c, slot)
        sends_done(slot)

        @pl.when(jnp.logical_not(first))
        def _():
            for cp in y_copies(t - 1, slot):
                cp.wait()

        @pl.when(jnp.logical_not(last))
        def _():
            for cp in x_copies(t + 1, nxt):
                cp.start()

        for c in range(CHUNKS):
            finish(c, slot, nxt)

            @pl.when(jnp.logical_not(last))
            def _():
                send_own(c, nxt)
        refill(7)
        refill(8)
        for cp in y_copies(t, nxt):
            cp.start()
        return carry

    lax.fori_loop(0, steps, step, 0)
    end = steps % 2
    hl_copy = pltpu.make_async_copy(acc.at[:, pl.ds(0, units)], hl_ref, loc_sem.at[0])
    cl_copy = pltpu.make_async_copy(cst, cl_ref, loc_sem.at[1])
    hl_copy.start()
    cl_copy.start()
    for cp in y_copies(steps - 1, end):
        cp.wait()
    hl_copy.wait()
    cl_copy.wait()


def solution(mesh):
    n = mesh.shape["model"]

    def local_fn(x, w_in, w_rec, gate_bias, h_init, c_init):
        in_dim, hidden = w_in.shape[0], w_rec.shape[0]
        units = w_rec.shape[2]
        rows, steps = x.shape[0], x.shape[1]
        half = units // 2
        assert in_dim == units and n == 8
        anyspec = pl.BlockSpec(memory_space=pl.ANY)
        dma = pltpu.SemaphoreType.DMA
        y, h_last, c_last = pl.pallas_call(
            functools.partial(lstm_kernel, n, steps),
            name="lstm",
            out_shape=(
                jax.ShapeDtypeStruct((steps, rows, units), jnp.bfloat16),
                jax.ShapeDtypeStruct((rows, units), jnp.float32),
                jax.ShapeDtypeStruct((rows, units), jnp.float32),
            ),
            in_specs=[anyspec, anyspec, anyspec, pl.BlockSpec(memory_space=pltpu.VMEM), anyspec, anyspec],
            out_specs=(anyspec, anyspec, anyspec),
            scratch_shapes=[
                pltpu.VMEM((2 * (n + 1) * 2, rows, half), jnp.bfloat16),
                pltpu.VMEM((n + 1, half, 4 * units), jnp.bfloat16),
                pltpu.VMEM((NSLOT, half, 4 * units), jnp.bfloat16),
                pltpu.VMEM((rows, 4 * units), jnp.float32),
                pltpu.VMEM((rows, units), jnp.float32),
                dma((7, CHUNKS)),
                dma((2, 7, CHUNKS)),
                dma((n + 1,)),
                dma((NSLOT,)),
                dma((2,)),
                dma((2,)),
                dma((2,)),
            ],
            compiler_params=pltpu.CompilerParams(
                collective_id=0, has_side_effects=True, vmem_limit_bytes=67043328),
        )(jnp.swapaxes(x, 0, 1), w_in.reshape(in_dim, 4 * units), w_rec.reshape(hidden, 4 * units),
          gate_bias.reshape(1, 4 * units), h_init, c_init)
        return jnp.swapaxes(y, 0, 1), h_last, c_last

    return jax.shard_map(
        local_fn,
        mesh=mesh,
        in_specs=(P("data", None, None), P(None, None, "model"), P(None, None, "model"),
                  P(None, "model"), P("data", "model"), P("data", "model")),
        out_specs=(P("data", None, "model"), P("data", "model"), P("data", "model")),
        check_vma=False,
    )
```
